32 devices in a mesh: sp: 4 (over z), dp: 8 (over y, x, core).
Axes of the slice: x: 2, y: 2, z: 4, core: 2. Of those that a mesh axis runs over, the one named last changes fastest.
Arguments:
- hidden_in: bfloat16 [16384, 512], P(('dp', 'sp'))
- cu_seqlens: int32 [8, 9], P('dp')
- pos_ids: int32 [16384], P(('dp', 'sp'))
- w_qkv: bfloat16 [2, 512, 1536], replicated
- w_attn_out: bfloat16 [2, 512, 512], replicated
- w_mlp_in: bfloat16 [2, 512, 1536], replicated
- w_mlp_out: bfloat16 [2, 768, 512], replicated
- ln_attn: float32 [2, 512], replicated
- ln_mlp: float32 [2, 512], replicated
- d_out: bfloat16 [16384, 512], P(('dp', 'sp'))
Outputs:
- output 1: bfloat16 [16384, 512], P(('dp', 'sp'))
- output 2: bfloat16 [16384, 512], P(('dp', 'sp'))
- output 3: float32 [2, 512, 1536], replicated
- output 4: float32 [2, 512, 512], replicated
- output 5: float32 [2, 512, 1536], replicated
- output 6: float32 [2, 768, 512], replicated
- output 7: float32 [2, 512], replicated
- output 8: float32 [2, 512], replicated
All inputs are finite; a program needn't handle non-finite values.
Results may differ from the reference program's by a relative error of at most 0.02.
Values are sent between devices in bfloat16 or wider.
A program may use at most 1 GiB of HBM per device.

```python
import jax
import jax.numpy as jnp
from jax import lax

SEQ_SHARDS = 4
DATA_GROUPS = 8
TOK_DEV = 512
D_MODEL = 512
N_HEADS = 8
HEAD_DIM = 64
FF_DIM = 768
N_DOCS = 8
WINDOW_HALF = 64
THETA_GLOBAL = 160000
THETA_LOCAL = 10000
GROUP_TOKENS = SEQ_SHARDS * TOK_DEV
ALL_TOKENS = DATA_GROUPS * GROUP_TOKENS
QUERY_BLOCK = WINDOW_HALF
LN_EPS = 1e-5


def draw_bounds(cut_key):
    cut_points = jax.random.permutation(cut_key, GROUP_TOKENS - 1)[: N_DOCS - 1] + 1
    inner_cuts = jnp.sort(cut_points).astype(jnp.int32)
    return jnp.concatenate([jnp.zeros((1,), jnp.int32), inner_cuts, jnp.full((1,), GROUP_TOKENS, jnp.int32)])


def doc_index(bounds):
    token_idx = jnp.arange(GROUP_TOKENS)
    return jnp.sum((bounds[None, 1:N_DOCS] <= token_idx[:, None]).astype(jnp.int32), axis=1)


def positions_of(bounds):
    token_idx = jnp.arange(GROUP_TOKENS)
    return (token_idx - bounds[doc_index(bounds)]).astype(jnp.int32)


def setup_inputs(seed: int = 0) -> dict:
    key_list = jax.random.split(jax.random.key(seed), 10)
    bounds = jax.vmap(draw_bounds)(jax.random.split(key_list[0], DATA_GROUPS))
    pos_ids = jax.vmap(positions_of)(bounds).reshape(ALL_TOKENS)

    def weight(key_idx, shape, fan_in):
        return (jax.random.normal(key_list[key_idx], shape, jnp.float32) * fan_in ** -0.5).astype(jnp.bfloat16)

    return {
        'hidden_in': jax.random.normal(key_list[1], (ALL_TOKENS, D_MODEL), jnp.float32).astype(jnp.bfloat16),
        'cu_seqlens': bounds,
        'pos_ids': pos_ids,
        'w_qkv': weight(2, (2, D_MODEL, 3 * D_MODEL), D_MODEL),
        'w_attn_out': weight(3, (2, D_MODEL, D_MODEL), D_MODEL),
        'w_mlp_in': weight(4, (2, D_MODEL, 2 * FF_DIM), D_MODEL),
        'w_mlp_out': weight(5, (2, FF_DIM, D_MODEL), FF_DIM),
        'ln_attn': 1.0 + 0.25 * jax.random.normal(key_list[6], (2, D_MODEL), jnp.float32),
        'ln_mlp': 1.0 + 0.25 * jax.random.normal(key_list[7], (2, D_MODEL), jnp.float32),
        'd_out': jax.random.normal(key_list[8], (ALL_TOKENS, D_MODEL), jnp.float32).astype(jnp.bfloat16),
    }


def layer_norm(in_rows, gain_row):
    rows32 = in_rows.astype(jnp.float32)
    centered = rows32 - jnp.mean(rows32, axis=-1, keepdims=True)
    var_row = jnp.mean(centered * centered, axis=-1, keepdims=True)
    return (centered * lax.rsqrt(var_row + LN_EPS) * gain_row).astype(jnp.bfloat16)


def rope(head_rows, pos_grp, rope_base):
    half_dim = HEAD_DIM // 2
    inv_freq = rope_base ** (jnp.arange(half_dim).astype(jnp.float32) * (-2.0 / HEAD_DIM))
    angles = pos_grp.astype(jnp.float32)[:, None] * inv_freq[None, :]
    cos_tab = jnp.concatenate([jnp.cos(angles), jnp.cos(angles)], axis=-1)[:, None, :]
    sin_tab = jnp.concatenate([jnp.sin(angles), jnp.sin(angles)], axis=-1)[:, None, :]
    rows32 = head_rows.astype(jnp.float32)
    rotated = jnp.concatenate([-rows32[..., half_dim:], rows32[..., :half_dim]], axis=-1)
    return (rows32 * cos_tab + rotated * sin_tab).astype(jnp.bfloat16)


def attention(query_rows, key_rows, val_rows, doc_ids, windowed):
    n_tok = query_rows.shape[0]
    key_f = key_rows.astype(jnp.float32)
    val_f = val_rows.astype(jnp.float32)
    token_idx = jnp.arange(n_tok)

    def one_block(blk_start):
        q_blk = lax.dynamic_slice_in_dim(query_rows, blk_start, QUERY_BLOCK, 0).astype(jnp.float32)
        doc_blk = lax.dynamic_slice_in_dim(doc_ids, blk_start, QUERY_BLOCK, 0)
        scores = jnp.einsum('qhd,khd->hqk', q_blk, key_f) * (HEAD_DIM ** -0.5)
        allowed = doc_blk[:, None] == doc_ids[None, :]
        if windowed:
            q_idx = blk_start + jnp.arange(QUERY_BLOCK)
            allowed = allowed & (jnp.abs(q_idx[:, None] - token_idx[None, :]) <= WINDOW_HALF)
        scores = jnp.where(allowed[None], scores, -1e30)
        prob_bf = jax.nn.softmax(scores, axis=-1).astype(jnp.bfloat16)
        return jnp.einsum('hqk,khd->qhd', prob_bf.astype(jnp.float32), val_f).astype(jnp.bfloat16)

    starts = jnp.arange(n_tok // QUERY_BLOCK) * QUERY_BLOCK
    return lax.map(jax.checkpoint(one_block), starts).reshape(query_rows.shape)


def layer(x_rows, pos_grp, doc_ids, params, rope_base, windowed):
    w_qkv, w_proj, w_up, w_down, g_attn, g_mlp = params
    n_tok = x_rows.shape[0]
    h_attn = layer_norm(x_rows, g_attn)
    qkv_rows = jnp.dot(h_attn.astype(jnp.float32), w_qkv, preferred_element_type=jnp.float32).astype(jnp.bfloat16)
    qkv_rows = qkv_rows.reshape(n_tok, 3, N_HEADS, HEAD_DIM)
    query_rows = rope(qkv_rows[:, 0], pos_grp, rope_base)
    key_rows = rope(qkv_rows[:, 1], pos_grp, rope_base)
    att_rows = attention(query_rows, key_rows, qkv_rows[:, 2], doc_ids, windowed).reshape(n_tok, D_MODEL)
    x_mid = (x_rows.astype(jnp.float32) + jnp.dot(att_rows.astype(jnp.float32), w_proj, preferred_element_type=jnp.float32)).astype(jnp.bfloat16)
    h_mlp = layer_norm(x_mid, g_mlp)
    up_rows = jnp.dot(h_mlp.astype(jnp.float32), w_up, preferred_element_type=jnp.float32).astype(jnp.bfloat16)
    gate_in = up_rows.astype(jnp.float32)
    act_rows = (jax.nn.gelu(gate_in[:, :FF_DIM], approximate=False) * gate_in[:, FF_DIM:]).astype(jnp.bfloat16)
    return (x_mid.astype(jnp.float32) + jnp.dot(act_rows.astype(jnp.float32), w_down, preferred_element_type=jnp.float32)).astype(jnp.bfloat16)


def two_layers(x_rows, pos_grp, doc_ids, all_params):
    first_params = tuple(stack_w[0] for stack_w in all_params)
    second_params = tuple(stack_w[1] for stack_w in all_params)
    hidden = layer(x_rows, pos_grp, doc_ids, first_params, THETA_GLOBAL, False)
    return layer(hidden, pos_grp, doc_ids, second_params, THETA_LOCAL, True)


def reference(hidden_in, cu_seqlens, pos_ids, w_qkv, w_attn_out, w_mlp_in, w_mlp_out, ln_attn, ln_mlp, d_out):
    all_params = (w_qkv.astype(jnp.float32), w_attn_out.astype(jnp.float32), w_mlp_in.astype(jnp.float32), w_mlp_out.astype(jnp.float32), ln_attn, ln_mlp)
    x_groups = hidden_in.reshape(DATA_GROUPS, GROUP_TOKENS, D_MODEL)
    dy_groups = d_out.reshape(DATA_GROUPS, GROUP_TOKENS, D_MODEL)
    pos_groups = pos_ids.reshape(DATA_GROUPS, GROUP_TOKENS)

    def group_step(grad_sum, group_in):
        x_grp, dy_grp, pos_grp, cu_row = group_in
        doc_ids = doc_index(cu_row)

        def forward(x_rows, layer_params):
            return two_layers(x_rows, pos_grp, doc_ids, layer_params)

        y_grp, vjp_pull = jax.vjp(forward, x_grp, all_params)
        dx_grp, d_params = vjp_pull(dy_grp)
        grad_sum = jax.tree.map(jnp.add, grad_sum, d_params)
        return grad_sum, (y_grp, dx_grp)

    zero_grads = jax.tree.map(jnp.zeros_like, all_params)
    grads, (y_groups, dx_groups) = lax.scan(group_step, zero_grads, (x_groups, dy_groups, pos_groups, cu_seqlens))
    return (y_groups.reshape(ALL_TOKENS, D_MODEL), dx_groups.reshape(ALL_TOKENS, D_MODEL)) + tuple(grads)
```

```python
import functools
import math
import jax
import jax.numpy as jnp
from jax import lax
from jax.experimental import pallas as pl
from jax.experimental.pallas import tpu as pltpu
from jax.sharding import PartitionSpec as P

HEAD_DIM = 64
PAIR = 2 * HEAD_DIM
HALO = 128
WINDOW_HALF = 64
LN_EPS = 1e-5
NEG_BIG = -1e30
SCALE = HEAD_DIM ** -0.5
EXP_SCALE = SCALE * math.log2(math.e)
BASES = (160000.0, 10000.0)
BQ_GLOBAL, BK_GLOBAL = 256, 256
BLK_LOCAL = 128
NT = (((1,), (1,)), ((), ()))
NN = (((1,), (0,)), ((), ()))


def mm(a, b, dims):
    return lax.dot_general(a, b, dims, preferred_element_type=jnp.float32)


def cost(flops, bytes_accessed=1 << 20):
    return pl.CostEstimate(flops=int(flops), bytes_accessed=int(bytes_accessed), transcendentals=0)


def layer_norm(in_rows, gain_row):
    rows32 = in_rows.astype(jnp.float32)
    centered = rows32 - jnp.mean(rows32, axis=-1, keepdims=True)
    var_row = jnp.mean(centered * centered, axis=-1, keepdims=True)
    return (centered * lax.rsqrt(var_row + LN_EPS) * gain_row).astype(jnp.bfloat16)


def geglu(up_rows):
    ff_dim = up_rows.shape[-1] // 2
    gate_in = up_rows.astype(jnp.float32)
    return (jax.nn.gelu(gate_in[:, :ff_dim], approximate=False) * gate_in[:, ff_dim:]).astype(jnp.bfloat16)


def rope_tables(pos, base):
    half = HEAD_DIM // 2
    inv_freq = base ** (jnp.arange(half).astype(jnp.float32) * (-2.0 / HEAD_DIM))
    angles = pos.astype(jnp.float32)[:, None] * inv_freq[None, :]
    cos, sin = jnp.cos(angles), jnp.sin(angles)
    return jnp.concatenate([cos] * 4, axis=-1), jnp.concatenate([-sin, sin, -sin, sin], axis=-1)


def half_swap(tile):
    lane = lax.broadcasted_iota(jnp.int32, tile.shape, 1)
    return jnp.where(lane % HEAD_DIM < HEAD_DIM // 2, pltpu.roll(tile, PAIR - 32, 1), pltpu.roll(tile, 32, 1))


def rope_back(grad_bf, cos, sin):
    g = grad_bf.astype(jnp.float32)
    return (g * cos - half_swap(g) * sin).astype(jnp.bfloat16)


def qkv_tile(x, gain, w_ref, cos, sin, put):
    h = layer_norm(x, gain)
    d_model = x.shape[1]
    for col in range(0, 3 * d_model, 512):
        t = mm(h, w_ref[:, col:col + 512], NN).astype(jnp.bfloat16)
        if col >= 2 * d_model:
            put(col, t)
        else:
            for c in range(0, 512, PAIR):
                g = t[:, c:c + PAIR].astype(jnp.float32)
                put(col + c, (g * cos + half_swap(g) * sin).astype(jnp.bfloat16))


def qkv_body(x_ref, gain_ref, w_ref, cos_ref, sin_ref, out_ref):
    def put(col, tile):
        out_ref[:, col:col + tile.shape[1]] = tile

    qkv_tile(x_ref[:, :], gain_ref[:, :], w_ref, cos_ref[:, :], sin_ref[:, :], put)


def qkv_rope(x, gain, w, cos, sin):
    rows, d_model = x.shape
    blk = 256
    row_spec = lambda width: pl.BlockSpec((blk, width), lambda i: (i, 0))
    whole = lambda shape: pl.BlockSpec(shape, lambda i: (0, 0))
    return pl.pallas_call(
        qkv_body,
        grid=(rows // blk,),
        in_specs=[row_spec(d_model), whole((1, d_model)), whole(w.shape), row_spec(PAIR), row_spec(PAIR)],
        out_specs=row_spec(3 * d_model),
        out_shape=jax.ShapeDtypeStruct((rows, 3 * d_model), jnp.bfloat16),
        cost_estimate=cost(2 * rows * d_model * 3 * d_model),
        name="qkv_rope",
    )(x, gain[None, :], w, cos, sin)


def head_lanes(shape, h):
    lane = lax.broadcasted_iota(jnp.int32, shape, 1)
    return (lane >= h * HEAD_DIM) & (lane < (h + 1) * HEAD_DIM)


def keep_head(tile, h):
    return jnp.where(head_lanes(tile.shape, h), tile, jnp.zeros_like(tile))


def pair_select(first, second):
    shape = (first.shape[0], PAIR)
    return jnp.where(head_lanes(shape, 0), first, second)


def window_mask(doc_rows, doc_cols, row0, col0):
    ok = doc_rows == doc_cols
    diff = (row0 + lax.broadcasted_iota(jnp.int32, ok.shape, 0)) - (col0 + lax.broadcasted_iota(jnp.int32, ok.shape, 1))
    return ok & (jnp.abs(diff) <= WINDOW_HALF)


def fwd_body(sc_ref, q_ref, k_ref, v_ref, dq_ref, dk_ref, o_ref, lse_ref, s_buf, top_s, sum_s, acc_s):
    i = pl.program_id(0)
    bk = s_buf.shape[3]
    lo, hi = sc_ref[1 + 2 * i], sc_ref[2 + 2 * i]
    q = q_ref[:, :]
    qh = [keep_head(q, h) for h in range(2)]
    doc_q = dq_ref[:, :]
    top_s[:, :, :] = jnp.full_like(top_s, NEG_BIG)
    sum_s[:, :, :] = jnp.zeros_like(sum_s)
    acc_s[:, :, :] = jnp.zeros_like(acc_s)

    def fold(op, tile):
        parts = [tile[:, c:c + PAIR] for c in range(0, bk, PAIR)]
        return functools.reduce(op, parts)

    def scores(kb, carry):
        k = k_ref[pl.ds(pl.multiple_of(kb * bk, bk), bk), :]
        ok = doc_q == dk_ref[kb]
        for h in range(2):
            s = jnp.where(ok, mm(qh[h], k, NT), NEG_BIG)
            s_buf[h, kb] = s
            top_s[h] = jnp.maximum(top_s[h], fold(jnp.maximum, s))
        return carry

    lax.fori_loop(lo, hi, scores, 0)
    shift = [jnp.max(top_s[h], axis=1, keepdims=True) * EXP_SCALE for h in range(2)]

    def values(kb, carry):
        v = v_ref[pl.ds(pl.multiple_of(kb * bk, bk), bk), :]
        for h in range(2):
            e = jnp.exp2(s_buf[h, kb] * EXP_SCALE - shift[h])
            sum_s[h] = sum_s[h] + fold(jnp.add, e)
            acc_s[h] = acc_s[h] + mm(e.astype(jnp.bfloat16), v, NN)
        return carry

    lax.fori_loop(lo, hi, values, 0)
    total = [jnp.sum(sum_s[h], axis=1, keepdims=True) for h in range(2)]
    o_ref[:, :] = pair_select(*[acc_s[h] / total[h] for h in range(2)]).astype(jnp.bfloat16)
    lse_ref[:, :] = pair_select(*[shift[h] + jnp.log2(total[h]) for h in range(2)])


def attn_fwd(scal, qkv, doc, n_blocks, bq, bk):
    rows, n_pairs = qkv.shape[0], qkv.shape[1] // 3 // PAIR
    doc_col, doc_row = doc[:, None], doc.reshape(rows // bk, 1, bk)
    n_out = n_blocks * bq
    qspec = pl.BlockSpec((bq, PAIR), lambda i, p, sc: (sc[0] + i, p))
    full = lambda part: pl.BlockSpec((rows, PAIR), lambda i, p, sc: (0, part * n_pairs + p))
    out = pl.BlockSpec((bq, PAIR), lambda i, p, sc: (i, p))
    return pl.pallas_call(
        fwd_body,
        grid_spec=pltpu.PrefetchScalarGridSpec(
            num_scalar_prefetch=1, grid=(n_blocks, n_pairs),
            in_specs=[qspec, full(1), full(2),
                      pl.BlockSpec((bq, 1), lambda i, p, sc: (sc[0] + i, 0)),
                      pl.BlockSpec((rows // bk, 1, bk), lambda i, p, sc: (0, 0, 0))],
            out_specs=[out, out],
            scratch_shapes=[pltpu.VMEM((2, rows // bk, bq, bk), jnp.float32)] + [pltpu.VMEM((2, bq, PAIR), jnp.float32)] * 3),
        out_shape=[jax.ShapeDtypeStruct((n_out, n_pairs * PAIR), jnp.bfloat16),
                   jax.ShapeDtypeStruct((n_out, n_pairs * PAIR), jnp.float32)],
        cost_estimate=cost(4e9),
        name="attn_fwd_global",
    )(scal, qkv, qkv, qkv, doc_col, doc_row)


def stats_body(o_ref, do_ref, lse_ref, out_ref):
    n = o_ref.shape[0]
    lane = lax.broadcasted_iota(jnp.int32, (n, PAIR), 1)
    tile = jnp.zeros((n, PAIR), jnp.float32)
    for p in range(o_ref.shape[1] // PAIR):
        cols = slice(p * PAIR, (p + 1) * PAIR)
        prod = o_ref[:, cols].astype(jnp.float32) * do_ref[:, cols].astype(jnp.float32)
        lse = lse_ref[:, cols]
        for h in range(2):
            delta = jnp.sum(jnp.where(head_lanes((n, PAIR), h), prod, 0.0), axis=1, keepdims=True)
            tile = jnp.where(lane == 8 * p + h, delta, tile)
            tile = jnp.where(lane == 8 * p + 2 + h, lse[:, h * HEAD_DIM:h * HEAD_DIM + 1], tile)
    out_ref[:, :] = tile.T[:out_ref.shape[0], :]


def attn_stats(o, do, lse):
    n, d_model = o.shape
    n_pairs = d_model // PAIR
    return pl.pallas_call(
        stats_body,
        out_shape=jax.ShapeDtypeStruct((8 * n_pairs, n), jnp.float32),
        cost_estimate=cost(1e8),
        name="attn_stats",
    )(o, do, lse)


def local_window(sc_ref, blk, n_blocks):
    i = pl.program_id(0) + sc_ref[0]
    return i * blk, pl.multiple_of(jnp.clip(i - 1, 0, n_blocks - 3) * blk, blk)


def local_fwd_body(blk, n_blocks, sc_ref, q_ref, kv_ref, dq_ref, dk_ref, o_ref, lse_ref):
    d_model = q_ref.shape[1]
    row0, start = local_window(sc_ref, blk, n_blocks)
    ok = window_mask(dq_ref[...], dk_ref[jnp.clip(pl.program_id(0) + sc_ref[0] - 1, 0, n_blocks - 3)], row0, start)
    for p in range(d_model // PAIR):
        cols = slice(p * PAIR, (p + 1) * PAIR)
        q = q_ref[:, cols]
        k = kv_ref[pl.ds(start, 3 * blk), d_model + p * PAIR:d_model + (p + 1) * PAIR]
        v = kv_ref[pl.ds(start, 3 * blk), 2 * d_model + p * PAIR:2 * d_model + (p + 1) * PAIR]
        outs, lses = [], []
        for h in range(2):
            s = jnp.where(ok, mm(keep_head(q, h), k, NT), NEG_BIG)
            top = jnp.max(s, axis=1, keepdims=True)
            e = jnp.exp2((s - top) * EXP_SCALE)
            total = jnp.sum(e, axis=1, keepdims=True)
            outs.append(mm(e.astype(jnp.bfloat16), v, NN) / total)
            lses.append(top * EXP_SCALE + jnp.log2(total))
        o_ref[:, cols] = pair_select(*outs).astype(jnp.bfloat16)
        lse_ref[:, cols] = pair_select(*lses)


def local_docs(doc, blk):
    windows = doc.shape[0] // blk - 2
    return jnp.stack([doc[i * blk:(i + 3) * blk] for i in range(windows)])[:, None, :]


def local_fwd(scal, qkv, doc, n_blocks, blk):
    rows, width = qkv.shape
    d_model = width // 3
    total = rows // blk
    out = pl.BlockSpec((blk, d_model), lambda i, sc: (i, 0))
    return pl.pallas_call(
        functools.partial(local_fwd_body, blk, total),
        grid_spec=pltpu.PrefetchScalarGridSpec(
            num_scalar_prefetch=1, grid=(n_blocks,),
            in_specs=[pl.BlockSpec((blk, d_model), lambda i, sc: (sc[0] + i, 0)),
                      pl.BlockSpec((rows, width), lambda i, sc: (0, 0)),
                      pl.BlockSpec((blk, 1), lambda i, sc: (sc[0] + i, 0)),
                      pl.BlockSpec((total - 2, 1, 3 * blk), lambda i, sc: (0, 0, 0))],
            out_specs=[out, out]),
        out_shape=[jax.ShapeDtypeStruct((n_blocks * blk, d_model), jnp.bfloat16),
                   jax.ShapeDtypeStruct((n_blocks * blk, d_model), jnp.float32)],
        cost_estimate=cost(1e9),
        name="local_fwd",
    )(scal, qkv, qkv, doc[:, None], local_docs(doc, blk))


def local_bwd_body(blk, n_blocks, sc_ref, own_ref, all_ref, o_ref, do_ref, lse_ref, doall_ref, st_ref, dq_ref, dk_ref, cos_ref, sin_ref, out_ref):
    d_model = o_ref.shape[1]
    row0, start = local_window(sc_ref, blk, n_blocks)
    ok = window_mask(dq_ref[...], dk_ref[jnp.clip(pl.program_id(0) + sc_ref[0] - 1, 0, n_blocks - 3)], row0, start)
    cos, sin = cos_ref[...], sin_ref[...]
    near = pl.ds(start, 3 * blk)
    for p in range(d_model // PAIR):
        cols = slice(p * PAIR, (p + 1) * PAIR)
        kcols = slice(d_model + p * PAIR, d_model + (p + 1) * PAIR)
        vcols = slice(2 * d_model + p * PAIR, 2 * d_model + (p + 1) * PAIR)
        q, k, v, do = own_ref[:, cols], own_ref[:, kcols], own_ref[:, vcols], do_ref[:, cols]
        qw, kw, vw, dow = all_ref[near, cols], all_ref[near, kcols], all_ref[near, vcols], doall_ref[near, cols]
        st = st_ref[jnp.clip(pl.program_id(0) + sc_ref[0] - 1, 0, n_blocks - 3), 8 * p:8 * p + 8, :]
        prod = o_ref[:, cols].astype(jnp.float32) * do.astype(jnp.float32)
        dqs, dks, dvs = [], [], []
        for h in range(2):
            delta = jnp.sum(keep_head(prod, h), axis=1, keepdims=True)
            lse = lse_ref[:, p * PAIR + h * HEAD_DIM:p * PAIR + h * HEAD_DIM + 1]
            s = mm(keep_head(q, h), kw, NT)
            prob = jnp.exp2(jnp.where(ok, s * EXP_SCALE - lse, NEG_BIG))
            dp = mm(keep_head(do, h), vw, NT).astype(jnp.bfloat16).astype(jnp.float32)
            dqs.append(mm((prob * (dp - delta)).astype(jnp.bfloat16), kw, NN))
            s = mm(keep_head(k, h), qw, NT)
            prob = jnp.exp2(jnp.where(ok, s * EXP_SCALE - st[2 + h:3 + h, :], NEG_BIG))
            dvs.append(mm(prob.astype(jnp.bfloat16), dow, NN))
            dp = mm(keep_head(v, h), dow, NT).astype(jnp.bfloat16).astype(jnp.float32)
            dks.append(mm((prob * (dp - st[h:h + 1, :])).astype(jnp.bfloat16), qw, NN))
        out_ref[:, cols] = rope_back((pair_select(*dqs) * SCALE).astype(jnp.bfloat16), cos, sin)
        out_ref[:, kcols] = rope_back((pair_select(*dks) * SCALE).astype(jnp.bfloat16), cos, sin)
        out_ref[:, vcols] = pair_select(*dvs).astype(jnp.bfloat16)


def local_bwd(scal, qkv, o, do, lse, stats, doc, cos, sin, n_blocks, blk):
    rows, width = qkv.shape
    d_model = width // 3
    total = rows // blk
    own = pl.BlockSpec((blk, d_model), lambda i, sc: (sc[0] + i, 0))
    table = pl.BlockSpec((blk, PAIR), lambda i, sc: (sc[0] + i, 0))
    whole = lambda w: pl.BlockSpec((rows, w), lambda i, sc: (0, 0))
    st = jnp.stack([stats[:, i * blk:(i + 3) * blk] for i in range(total - 2)])
    return pl.pallas_call(
        functools.partial(local_bwd_body, blk, total),
        grid_spec=pltpu.PrefetchScalarGridSpec(
            num_scalar_prefetch=1, grid=(n_blocks,),
            in_specs=[pl.BlockSpec((blk, width), lambda i, sc: (sc[0] + i, 0)), whole(width), own, own, own, whole(d_model),
                      pl.BlockSpec(st.shape, lambda i, sc: (0, 0, 0)),
                      pl.BlockSpec((blk, 1), lambda i, sc: (sc[0] + i, 0)),
                      pl.BlockSpec((total - 2, 1, 3 * blk), lambda i, sc: (0, 0, 0)), table, table],
            out_specs=pl.BlockSpec((blk, width), lambda i, sc: (i, 0))),
        out_shape=jax.ShapeDtypeStruct((n_blocks * blk, width), jnp.bfloat16),
        cost_estimate=cost(2e9),
        name="local_bwd",
    )(scal, qkv, qkv, o, do, lse, do, st, doc[:, None], local_docs(doc, blk), cos, sin)


STEP_AXIS = {'c': ('dp', 1), 'x': ('dp', 2), 'y': ('dp', 4), 'Z': ('sp', 2), 'z': ('sp', 1)}
A_WAY, B_WAY, C_WAY = 'cxyzZ', 'cyxzZ', 'czZxy'


def partner_of(step):
    axis, bit = STEP_AXIS[step]
    me = lax.axis_index(axis)
    low = (me // bit) % 2
    return {axis: me + bit - 2 * bit * low}, low


def plan_chunks(shapes, ways):
    by_way = {way: [] for way in (A_WAY, B_WAY, C_WAY)}
    for idx, ((rows, cols), way) in enumerate(zip(shapes, ways)):
        parts = 1 if way == C_WAY else 2
        for part in range(parts):
            by_way[way].append((idx, part * rows // parts, rows // parts, cols, way))
    return [chunk for group in zip(*by_way.values()) for chunk in group]


GRAD_WAYS = (A_WAY, B_WAY, C_WAY, C_WAY)
STAGGER = 1
MESH_ID = pl.DeviceIdType.MESH
N_STEPS = len(A_WAY)


def greet(peers):
    barrier = pltpu.get_barrier_semaphore()
    for peer in peers:
        pl.semaphore_signal(barrier, inc=1, device_id=peer, device_id_type=MESH_ID)
    pl.semaphore_wait(barrier, len(peers))


def sum_waves(chunks, ins, outs, scratch):
    n_ch = len(chunks)
    lands, works, (load_sem, send_sem, recv_sem) = scratch[:n_ch], scratch[n_ch:2 * n_ch], scratch[2 * n_ch:]
    loads = [pltpu.make_async_copy(ins[idx].at[pl.ds(first, rows)], works[j], load_sem.at[j])
             for j, (idx, first, rows, _, _) in enumerate(chunks)]
    for copy in loads:
        copy.start()
    base = [0] * n_ch
    size = [c[2] for c in chunks]
    land_at = [0] * n_ch
    pending = [None] * n_ch
    sends = []

    def advance(j, s):
        idx, first, _, _, way = chunks[j]
        out = outs[idx]
        if s == 0:
            loads[j].wait()
        else:
            copy, keep, half, at = pending[j]
            copy.wait_recv()
            if s <= N_STEPS:
                @pl.loop(0, half // 8)
                def _(r):
                    rows = pl.ds(pl.multiple_of(keep + r * 8, 8), 8)
                    total = works[j][rows, :] + lands[j][pl.ds(pl.multiple_of(at + r * 8, 8), 8), :]
                    if s < N_STEPS:
                        works[j][rows, :] = total
                    else:
                        out[pl.ds(pl.multiple_of(first + keep + r * 8, 8), 8), :] = total
        if s == 2 * N_STEPS:
            return
        peer, low = partner_of((way + way[::-1])[s])
        if s < N_STEPS:
            half = size[j] // 2
            give = pl.multiple_of(base[j] + (1 - low) * half, 8)
            keep = pl.multiple_of(base[j] + low * half, 8)
            source, target = works[j].at[pl.ds(give, half)], lands[j].at[pl.ds(land_at[j], half)]
            after = (keep, half, land_at[j])
            land_at[j] += half
            base[j], size[j] = keep, half
        else:
            rows = pl.ds(pl.multiple_of(first + base[j], 8), size[j])
            source = target = out.at[rows]
            after = (None, None, None)
            base[j] = pl.multiple_of(base[j] - low * size[j], 8)
            size[j] *= 2
        copy = pltpu.make_async_remote_copy(
            src_ref=source, dst_ref=target, send_sem=send_sem.at[j, s], recv_sem=recv_sem.at[j, s],
            device_id=peer, device_id_type=MESH_ID)
        copy.start()
        sends.append(copy)
        pending[j] = (copy,) + after

    def wave(w):
        for j in range(n_ch):
            s = w - (j // 3) * STAGGER
            if 0 <= s <= 2 * N_STEPS:
                advance(j, s)

    def finish():
        for copy in sends:
            copy.wait_send()

    n_waves = 2 * N_STEPS + 1 + (n_ch - 1) // 3 * STAGGER
    return [functools.partial(wave, w) for w in range(n_waves)], finish


def sum_scratch(chunks):
    n_ch = len(chunks)
    dma = pltpu.SemaphoreType.DMA
    return [pltpu.VMEM((c[2], c[3]), jnp.float32) for c in chunks] * 2 + [dma((n_ch,))] + [dma((n_ch, 2 * N_STEPS))] * 2


def sum_body(chunks, n_arr, *refs):
    ins, gain_in = refs[:n_arr], refs[n_arr]
    outs, (gain_out, gain_land, gsend_sem, grecv_sem) = refs[n_arr + 1:2 * n_arr + 1], refs[2 * n_arr + 1:2 * n_arr + 5]
    waves, finish = sum_waves(chunks, ins, outs, refs[2 * n_arr + 5:])
    greet([partner_of(step)[0] for step in A_WAY])
    gain_out[:, :] = gain_in[:, :]
    pending = []
    for w, wave in enumerate(waves):
        wave()
        if pending:
            pending.pop().wait()
            gain_out[:, :] = gain_out[:, :] + gain_land[w - 1]
        if w < N_STEPS:
            copy = pltpu.make_async_remote_copy(
                src_ref=gain_out, dst_ref=gain_land.at[w], send_sem=gsend_sem.at[w], recv_sem=grecv_sem.at[w],
                device_id=partner_of(A_WAY[w])[0], device_id_type=MESH_ID)
            copy.start()
            pending.append(copy)
    finish()


def sum_all(grads, gains, collective_id):
    chunks = plan_chunks([g.shape for g in grads], GRAD_WAYS)
    n_arr = len(grads)
    vmem = pl.BlockSpec(memory_space=pltpu.VMEM)
    res = pl.pallas_call(
        functools.partial(sum_body, chunks, n_arr),
        in_specs=[pl.BlockSpec(memory_space=pl.ANY)] * n_arr + [vmem],
        out_specs=[vmem] * (n_arr + 1),
        out_shape=[jax.ShapeDtypeStruct(g.shape, jnp.float32) for g in grads + [gains]],
        scratch_shapes=[pltpu.VMEM((N_STEPS,) + gains.shape, jnp.float32), pltpu.SemaphoreType.DMA((N_STEPS,)),
                        pltpu.SemaphoreType.DMA((N_STEPS,))] + sum_scratch(chunks),
        compiler_params=pltpu.CompilerParams(collective_id=collective_id, has_side_effects=True, vmem_limit_bytes=60 << 20),
        cost_estimate=cost(1e10),
        name="grad_sum",
    )(*grads, gains)
    return res[:-1], res[-1]


def line_rounds(n_dev, ins, outs, send_sem, recv_sem):
    me = lax.axis_index('sp')
    has = (me < n_dev - 1, me > 0)
    arrays = range(len(ins))

    def owner_of(side, d):
        return me - d if side == 0 else me + d

    def exists(side, d):
        return owner_of(0, d) >= 0 if side == 0 else owner_of(1, d) < n_dev

    def copy(side, d, a, source):
        owner = owner_of(side, d)
        return pltpu.make_async_remote_copy(
            src_ref=source if source is not None else outs[a].at[owner], dst_ref=outs[a].at[owner],
            send_sem=send_sem.at[side, d, a], recv_sem=recv_sem.at[side, d, a],
            device_id={'sp': owner_of(side, -1)} if side == 0 else {'sp': me - 1}, device_id_type=MESH_ID)

    def came(side, d, a):
        owner = owner_of(side, d)
        return pltpu.make_async_remote_copy(
            src_ref=outs[a].at[owner], dst_ref=outs[a].at[owner], send_sem=send_sem.at[side, d - 1, a],
            recv_sem=recv_sem.at[side, d - 1, a], device_id={'sp': me}, device_id_type=MESH_ID)

    def first():
        for a in arrays:
            for side in range(2):
                @pl.when(has[side])
                def _():
                    copy(side, 0, a, ins[a]).start()
        for a in arrays:
            outs[a][me] = ins[a][:, :]

    def relay(d):
        for a in arrays:
            for side in range(2):
                @pl.when(exists(side, d))
                def _():
                    came(side, d, a).wait_recv()
                if d < n_dev - 1:
                    @pl.when(exists(side, d) & has[side])
                    def _():
                        copy(side, d, a, None).start()

    def finish():
        for d in range(n_dev - 1):
            for a in arrays:
                for side in range(2):
                    @pl.when(exists(side, d) & has[side])
                    def _():
                        copy(side, d, a, None if d else ins[a]).wait_send()

    return [first] + [functools.partial(relay, d) for d in range(1, n_dev)], finish


def other_shards(n_dev):
    me = lax.axis_index('sp')
    return [{'sp': lax.rem(me + d, n_dev)} for d in range(1, n_dev)]


def gather_qkv_body(n_dev, blk, x_ref, gain_ref, w_ref, cos_ref, sin_ref, out_ref, x_all, send_sem, recv_sem):
    rounds, finish = line_rounds(n_dev, (x_ref,), (x_all,), send_sem, recv_sem)
    me = lax.axis_index('sp')
    n_loc = x_ref.shape[0]
    greet(other_shards(n_dev))

    def shard_qkv(owner):
        @pl.loop(0, n_loc // blk)
        def _(i):
            rows = pl.ds(pl.multiple_of(i * blk, blk), blk)
            table = pl.ds(pl.multiple_of(owner * n_loc + i * blk, blk), blk)

            def put(col, tile):
                out_ref[owner, rows, col:col + tile.shape[1]] = tile

            qkv_tile(x_all[owner, rows, :], gain_ref[:, :], w_ref, cos_ref[table, :], sin_ref[table, :], put)

    rounds[0]()
    shard_qkv(me)
    for d in range(1, n_dev):
        rounds[d]()

        @pl.loop(0, 2)
        def _(side):
            owner = me - d + side * 2 * d

            @pl.when((owner >= 0) & (owner < n_dev))
            def _():
                shard_qkv(owner)
    finish()


def gather_qkv(x, gain, w, cos, sin, n_dev, collective_id):
    vmem = pl.BlockSpec(memory_space=pltpu.VMEM)
    rows, d_model = x.shape
    out = pl.pallas_call(
        functools.partial(gather_qkv_body, n_dev, 256),
        in_specs=[vmem] * 5, out_specs=vmem,
        out_shape=jax.ShapeDtypeStruct((n_dev, rows, 3 * d_model), jnp.bfloat16),
        scratch_shapes=[pltpu.VMEM((n_dev,) + x.shape, x.dtype)] + [pltpu.SemaphoreType.DMA((2, n_dev - 1, 1))] * 2,
        compiler_params=pltpu.CompilerParams(collective_id=collective_id, has_side_effects=True),
        cost_estimate=cost(1e10),
        name="gather_qkv",
    )(x, gain[None, :], w, cos, sin)
    return out.reshape(n_dev * rows, 3 * d_model)


def bwd_body(n_dev, blk, chunks, n_arr, *refs):
    qkv_ref, o_ref, do_ref, lse_ref, st_ref, doc_own, doc_row, cos_ref, sin_ref = refs[:9]
    rest = refs[9:]
    ins, out_ref, outs = rest[:n_arr], rest[n_arr], rest[n_arr + 1:2 * n_arr + 1]
    do_all, st_all, first_s, second_s, lsend, lrecv = rest[2 * n_arr + 1:2 * n_arr + 7]
    waves, sums_done = sum_waves(chunks, ins, outs, rest[2 * n_arr + 7:])
    rounds, line_done = line_rounds(n_dev, (do_ref, st_ref), (do_all, st_all), lsend, lrecv)
    me = lax.axis_index('sp')
    n_loc, d_model = o_ref.shape
    n_blk = n_dev * n_loc // blk
    per_shard = n_loc // blk
    greet([partner_of(step)[0] for step in 'cxy'] + other_shards(n_dev))
    rounds[0]()

    def tiles(p, i):
        rows = pl.ds(i * blk, blk)
        group = pl.ds(pl.multiple_of(me * n_loc + i * blk, blk), blk)
        cols = [slice(part * d_model + p * PAIR, part * d_model + (p + 1) * PAIR) for part in range(3)]
        return rows, group, cols

    def dq_unit(p, i):
        rows, group, (qc, kc, vc) = tiles(p, i)
        q, do = qkv_ref[group, qc], do_ref[rows, qc]
        prod = o_ref[rows, qc].astype(jnp.float32) * do.astype(jnp.float32)
        qh = [keep_head(q, h) for h in range(2)]
        doh = [keep_head(do, h) for h in range(2)]
        delta = [jnp.sum(keep_head(prod, h), axis=1, keepdims=True) for h in range(2)]
        lse = [lse_ref[rows, p * PAIR + h * HEAD_DIM:p * PAIR + h * HEAD_DIM + 1] for h in range(2)]
        doc = doc_own[rows, :]
        first_s[:, :] = jnp.zeros_like(first_s)

        def step(kb, carry):
            near = pl.ds(pl.multiple_of(kb * blk, blk), blk)
            k, v = qkv_ref[near, kc], qkv_ref[near, vc]
            ok = doc == doc_row[kb]
            parts = []
            for h in range(2):
                prob = jnp.exp2(jnp.where(ok, mm(qh[h], k, NT) * EXP_SCALE - lse[h], NEG_BIG))
                dp = mm(doh[h], v, NT).astype(jnp.bfloat16).astype(jnp.float32)
                parts.append(mm((prob * (dp - delta[h])).astype(jnp.bfloat16), k, NN))
            first_s[:, :] += pair_select(*parts)
            return carry

        lax.fori_loop(0, n_blk, step, 0)
        out_ref[rows, qc] = rope_back((first_s[:, :] * SCALE).astype(jnp.bfloat16), cos_ref[rows, :], sin_ref[rows, :])

    def dkv_unit(p, i):
        rows, group, (qc, kc, vc) = tiles(p, i)
        kh = [keep_head(qkv_ref[group, kc], h) for h in range(2)]
        vh = [keep_head(qkv_ref[group, vc], h) for h in range(2)]
        doc = doc_own[rows, :]
        first_s[:, :] = jnp.zeros_like(first_s)
        second_s[:, :] = jnp.zeros_like(second_s)

        def step(qb, carry):
            near = pl.ds(pl.multiple_of(qb * blk, blk), blk)
            part = pl.ds(pl.multiple_of(qb % per_shard * blk, blk), blk)
            q, do = qkv_ref[near, qc], do_all[qb // per_shard, part, qc]
            st = st_all[qb // per_shard, 8 * p:8 * p + 8, part]
            ok = doc == doc_row[qb]
            dks, dvs = [], []
            for h in range(2):
                prob = jnp.exp2(jnp.where(ok, mm(kh[h], q, NT) * EXP_SCALE - st[2 + h:3 + h, :], NEG_BIG))
                dvs.append(mm(prob.astype(jnp.bfloat16), do, NN))
                dp = mm(vh[h], do, NT).astype(jnp.bfloat16).astype(jnp.float32)
                dks.append(mm((prob * (dp - st[h:h + 1, :])).astype(jnp.bfloat16), q, NN))
            first_s[:, :] += pair_select(*dks)
            second_s[:, :] += pair_select(*dvs)
            return carry

        lax.fori_loop(0, n_blk, step, 0)
        out_ref[rows, kc] = rope_back((first_s[:, :] * SCALE).astype(jnp.bfloat16), cos_ref[rows, :], sin_ref[rows, :])
        out_ref[rows, vc] = second_s[:, :].astype(jnp.bfloat16)

    where = [(p, i) for p in range(d_model // PAIR) for i in range(per_shard)]
    units = [functools.partial(dq_unit, *at) for at in where] + [functools.partial(dkv_unit, *at) for at in where]
    turn = 0
    for n, unit in enumerate(units):
        if n == len(where):
            for step in rounds[len(rounds) - 1:]:
                step()
        unit()
        if n % 2 and n // 2 + 1 < len(rounds) - 1:
            rounds[n // 2 + 1]()
        while turn < len(waves) and turn * len(units) <= n * len(waves):
            waves[turn]()
            turn += 1
    line_done()
    sums_done()


def bwd_global(qkv, o, do, lse, stats, doc_own, doc_row, cos, sin, grads, n_dev, blk, collective_id):
    chunks = plan_chunks([g.shape for g in grads], GRAD_WAYS)
    n_arr = len(grads)
    vmem = pl.BlockSpec(memory_space=pltpu.VMEM)
    n_loc, d_model = o.shape
    dma = pltpu.SemaphoreType.DMA
    res = pl.pallas_call(
        functools.partial(bwd_body, n_dev, blk, chunks, n_arr),
        in_specs=[vmem] * 9 + [pl.BlockSpec(memory_space=pl.ANY)] * n_arr,
        out_specs=[vmem] * (n_arr + 1),
        out_shape=[jax.ShapeDtypeStruct((n_loc, 3 * d_model), jnp.bfloat16)]
        + [jax.ShapeDtypeStruct(g.shape, jnp.float32) for g in grads],
        scratch_shapes=[pltpu.VMEM((n_dev,) + do.shape, do.dtype), pltpu.VMEM((n_dev,) + stats.shape, jnp.float32)]
        + [pltpu.VMEM((blk, PAIR), jnp.float32)] * 2 + [dma((2, n_dev - 1, 2))] * 2 + sum_scratch(chunks),
        compiler_params=pltpu.CompilerParams(collective_id=collective_id, has_side_effects=True, vmem_limit_bytes=63 << 20),
        cost_estimate=cost(1e10),
        name="bwd_global",
    )(qkv, o, do, lse, stats, doc_own, doc_row, cos, sin, *grads)
    return res[0], res[1:]


def weight_grad(left_rows, right_rows):
    return lax.dot_general(left_rows, right_rows, (((0,), (0,)), ((), ())), preferred_element_type=jnp.float32)


def input_grad(grad_rows, weight):
    return lax.dot_general(grad_rows, weight, (((1,), (1,)), ((), ())), preferred_element_type=jnp.float32).astype(jnp.bfloat16)


def solution(mesh):
    sp_size, dp_size = mesh.shape['sp'], mesh.shape['dp']
    token_spec = P(('dp', 'sp'), None)
    up_perm = [(i, i + 1) for i in range(sp_size - 1)]
    down_perm = [(i + 1, i) for i in range(sp_size - 1)]

    def with_halo(rows):
        left = lax.ppermute(rows[-HALO:], 'sp', up_perm)
        right = lax.ppermute(rows[:HALO], 'sp', down_perm)
        return jnp.concatenate([left, rows, right], axis=0)

    def device_step(x_loc, cu_loc, pos_loc, w_qkv, w_proj, w_up, w_down, ln_attn, ln_mlp, d_out):
        n_loc, d_model = x_loc.shape
        n_group = n_loc * sp_size
        me = lax.axis_index('sp')
        cu = cu_loc[0]
        tok = jnp.arange(n_group)
        doc_all = jnp.sum((cu[None, 1:-1] <= tok[:, None]).astype(jnp.int32), axis=1)
        pos_all = tok - cu[doc_all]
        tok_ext = me * n_loc - HALO + jnp.arange(n_loc + 2 * HALO)
        inside = (tok_ext >= 0) & (tok_ext < n_group)
        doc_at = jnp.sum((cu[None, 1:-1] <= tok_ext[:, None]).astype(jnp.int32), axis=1)
        doc_ext = jnp.where(inside, doc_at, -1)
        pos_ext = jnp.where(inside, tok_ext - cu[doc_at], 0)

        def bounds(blk, other):
            first = me * n_loc + jnp.arange(n_loc // blk) * blk
            lo = cu[doc_all[first]] // other
            hi = (cu[doc_all[first + blk - 1] + 1] + other - 1) // other
            pairs = jnp.stack([lo, hi], axis=1).reshape(-1)
            return jnp.concatenate([(me * n_loc // blk)[None], pairs]).astype(jnp.int32)

        sc_q = bounds(BQ_GLOBAL, BK_GLOBAL)
        n_ext = n_loc // BLK_LOCAL + 2 * (HALO // BLK_LOCAL)

        cos0, sin0 = rope_tables(pos_all, BASES[0])
        cos1, sin1 = rope_tables(pos_ext, BASES[1])

        def mlp_forward(x_rows, att, layer):
            x_mid = (x_rows.astype(jnp.float32) + jnp.dot(att, w_proj[layer], preferred_element_type=jnp.float32)).astype(jnp.bfloat16)
            h_mlp, ln2_pull = jax.vjp(layer_norm, x_mid, ln_mlp[layer])
            up_rows = jnp.dot(h_mlp, w_up[layer], preferred_element_type=jnp.float32).astype(jnp.bfloat16)
            act_rows, act_pull = jax.vjp(geglu, up_rows)
            y_rows = (x_mid.astype(jnp.float32) + jnp.dot(act_rows, w_down[layer], preferred_element_type=jnp.float32)).astype(jnp.bfloat16)
            return y_rows, (h_mlp, ln2_pull, act_pull, act_rows)

        def mlp_backward(d_y, saved, att, layer):
            h_mlp, ln2_pull, act_pull, act_rows = saved
            (d_up,) = act_pull(input_grad(d_y, w_down[layer]))
            d_mid_ln, g_ln = ln2_pull(input_grad(d_up, w_up[layer]))
            d_mid = d_y + d_mid_ln
            d_att = input_grad(d_mid, w_proj[layer])
            grads = (weight_grad(act_rows, d_y), weight_grad(h_mlp, d_up), weight_grad(att, d_mid))
            return d_mid, d_att, grads, g_ln

        qkv0 = gather_qkv(x_loc, ln_attn[0], w_qkv[0], cos0, sin0, sp_size, 0)
        att0, lse0 = attn_fwd(sc_q, qkv0, doc_all, n_loc // BQ_GLOBAL, BQ_GLOBAL, BK_GLOBAL)
        y0, saved0 = mlp_forward(x_loc, att0, 0)
        qkv1 = qkv_rope(with_halo(y0), ln_attn[1], w_qkv[1], cos1, sin1)
        att1x, lse1 = local_fwd(jnp.zeros((1,), jnp.int32), qkv1, doc_ext, n_ext, BLK_LOCAL)
        att1 = att1x[HALO:HALO + n_loc]
        y1, saved1 = mlp_forward(y0, att1, 1)

        def finish(d_qkv, x_rows, d_mid, layer):
            h_attn, ln1_pull = jax.vjp(layer_norm, x_rows, ln_attn[layer])
            g_qkv = weight_grad(h_attn, d_qkv)
            d_x_ln, g_ln = ln1_pull(input_grad(d_qkv, w_qkv[layer]))
            return d_mid + d_x_ln, g_qkv, g_ln

        d_mid1, d_att1, (g_down1, g_up1, g_proj1), g_lnm1 = mlp_backward(d_out, saved1, att1, 1)
        do_ext = with_halo(d_att1)
        stats1 = attn_stats(att1x, do_ext, lse1)
        d_qkv1 = local_bwd(jnp.ones((1,), jnp.int32), qkv1, att1x, do_ext, lse1, stats1, doc_ext, cos1, sin1, n_loc // BLK_LOCAL, BLK_LOCAL)
        d_y0, g_qkv1, g_lna1 = finish(d_qkv1, y0, d_mid1, 1)
        d_mid0, d_att0, (g_down0, g_up0, g_proj0), g_lnm0 = mlp_backward(d_y0, saved0, att0, 0)
        stats0 = attn_stats(att0, d_att0, lse0)
        own_rows = lambda table: lax.dynamic_slice_in_dim(table, me * n_loc, n_loc, 0)
        d_qkv0, (qkvg1, up1, down1, proj1) = bwd_global(
            qkv0, att0, d_att0, lse0, stats0, own_rows(doc_all[:, None]), doc_all.reshape(-1, 1, BK_GLOBAL),
            own_rows(cos0), own_rows(sin0), [g_qkv1, g_up1, g_down1, g_proj1], sp_size, BK_GLOBAL, 1)
        d_x, g_qkv0, g_lna0 = finish(d_qkv0, x_loc, d_mid0, 0)
        gains = jnp.concatenate([jnp.stack([g_lna0, g_lna1, g_lnm0, g_lnm1]), jnp.zeros((4, d_model), jnp.float32)])
        (qkvg0, up0, down0, proj0), gains = sum_all([g_qkv0, g_up0, g_down0, g_proj0], gains, 2)
        return (y1, d_x, jnp.stack([qkvg0, qkvg1]), jnp.stack([proj0, proj1]), jnp.stack([up0, up1]),
                jnp.stack([down0, down1]), gains[:2], gains[2:4])

    in_specs = (token_spec, P('dp', None), P(('dp', 'sp')), P(), P(), P(), P(), P(), P(), token_spec)
    out_specs = (token_spec, token_spec, P(), P(), P(), P(), P(), P())
    return jax.shard_map(device_step, mesh=mesh, in_specs=in_specs, out_specs=out_specs, check_vma=False)
```

```python
import functools
import math
import jax
import jax.numpy as jnp
from jax import lax
from jax.experimental import pallas as pl
from jax.experimental.pallas import tpu as pltpu
from jax.sharding import PartitionSpec as P

HEAD_DIM = 64
PAIR = 2 * HEAD_DIM
HALO = 128
WINDOW_HALF = 64
LN_EPS = 1e-5
NEG_BIG = -1e30
SCALE = HEAD_DIM ** -0.5
EXP_SCALE = SCALE * math.log2(math.e)
BASES = (160000.0, 10000.0)
BQ_GLOBAL, BK_GLOBAL = 256, 256
BLK_LOCAL = 128
NT = (((1,), (1,)), ((), ()))
NN = (((1,), (0,)), ((), ()))


def mm(a, b, dims):
    return lax.dot_general(a, b, dims, preferred_element_type=jnp.float32)


def cost(flops, bytes_accessed=1 << 20):
    return pl.CostEstimate(flops=int(flops), bytes_accessed=int(bytes_accessed), transcendentals=0)


def layer_norm(in_rows, gain_row):
    rows32 = in_rows.astype(jnp.float32)
    centered = rows32 - jnp.mean(rows32, axis=-1, keepdims=True)
    var_row = jnp.mean(centered * centered, axis=-1, keepdims=True)
    return (centered * lax.rsqrt(var_row + LN_EPS) * gain_row).astype(jnp.bfloat16)


def geglu(up_rows):
    ff_dim = up_rows.shape[-1] // 2
    gate_in = up_rows.astype(jnp.float32)
    return (jax.nn.gelu(gate_in[:, :ff_dim], approximate=False) * gate_in[:, ff_dim:]).astype(jnp.bfloat16)


def rope_tables(pos, base):
    half = HEAD_DIM // 2
    lane = jnp.arange(PAIR)
    inv_freq = base ** ((lane % half).astype(jnp.float32) * (-2.0 / HEAD_DIM))
    angles = pos.astype(jnp.float32)[:, None] * inv_freq[None, :]
    return jnp.cos(angles), jnp.where(lane[None, :] % HEAD_DIM < half, -jnp.sin(angles), jnp.sin(angles))


def half_swap(tile):
    lane = lax.broadcasted_iota(jnp.int32, tile.shape, 1)
    return jnp.where(lane % HEAD_DIM < HEAD_DIM // 2, pltpu.roll(tile, PAIR - 32, 1), pltpu.roll(tile, 32, 1))


def rope_back(grad_bf, cos, sin):
    g = grad_bf.astype(jnp.float32)
    return (g * cos - half_swap(g) * sin).astype(jnp.bfloat16)


def qkv_tile(x, gain, w_ref, cos, sin, put):
    h = layer_norm(x, gain)
    d_model = x.shape[1]
    for col in range(0, 3 * d_model, 512):
        t = mm(h, w_ref[:, col:col + 512], NN).astype(jnp.bfloat16)
        if col >= 2 * d_model:
            put(col, t)
        else:
            for c in range(0, 512, PAIR):
                g = t[:, c:c + PAIR].astype(jnp.float32)
                put(col + c, (g * cos + half_swap(g) * sin).astype(jnp.bfloat16))


def qkv_body(x_ref, gain_ref, w_ref, cos_ref, sin_ref, out_ref):
    def put(col, tile):
        out_ref[:, col:col + tile.shape[1]] = tile

    qkv_tile(x_ref[:, :], gain_ref[:, :], w_ref, cos_ref[:, :], sin_ref[:, :], put)


def qkv_rope(x, gain, w, cos, sin):
    rows, d_model = x.shape
    blk = 256
    row_spec = lambda width: pl.BlockSpec((blk, width), lambda i: (i, 0))
    whole = lambda shape: pl.BlockSpec(shape, lambda i: (0, 0))
    return pl.pallas_call(
        qkv_body,
        grid=(rows // blk,),
        in_specs=[row_spec(d_model), whole((1, d_model)), whole(w.shape), row_spec(PAIR), row_spec(PAIR)],
        out_specs=row_spec(3 * d_model),
        out_shape=jax.ShapeDtypeStruct((rows, 3 * d_model), jnp.bfloat16),
        cost_estimate=cost(2 * rows * d_model * 3 * d_model),
        name="qkv_rope",
    )(x, gain[None, :], w, cos, sin)


def head_lanes(shape, h):
    lane = lax.broadcasted_iota(jnp.int32, shape, 1)
    return (lane >= h * HEAD_DIM) & (lane < (h + 1) * HEAD_DIM)


def keep_head(tile, h):
    return jnp.where(head_lanes(tile.shape, h), tile, jnp.zeros_like(tile))


def pair_select(first, second):
    shape = (first.shape[0], PAIR)
    return jnp.where(head_lanes(shape, 0), first, second)


def window_mask(doc_rows, doc_cols, row0, col0):
    ok = doc_rows == doc_cols
    diff = (row0 + lax.broadcasted_iota(jnp.int32, ok.shape, 0)) - (col0 + lax.broadcasted_iota(jnp.int32, ok.shape, 1))
    return ok & (jnp.abs(diff) <= WINDOW_HALF)


def fwd_body(sc_ref, q_ref, k_ref, v_ref, dq_ref, dk_ref, o_ref, lse_ref, s_buf, top_s, sum_s, acc_s):
    i = pl.program_id(0)
    bk = s_buf.shape[3]
    lo, hi = sc_ref[1 + 2 * i], sc_ref[2 + 2 * i]
    q = q_ref[:, :]
    qh = [keep_head(q, h) for h in range(2)]
    doc_q = dq_ref[:, :]
    top_s[:, :, :] = jnp.full_like(top_s, NEG_BIG)
    sum_s[:, :, :] = jnp.zeros_like(sum_s)
    acc_s[:, :, :] = jnp.zeros_like(acc_s)

    def fold(op, tile):
        parts = [tile[:, c:c + PAIR] for c in range(0, bk, PAIR)]
        return functools.reduce(op, parts)

    def scores(kb, carry):
        k = k_ref[pl.ds(pl.multiple_of(kb * bk, bk), bk), :]
        ok = doc_q == dk_ref[kb]
        for h in range(2):
            s = jnp.where(ok, mm(qh[h], k, NT), NEG_BIG)
            s_buf[h, kb] = s
            top_s[h] = jnp.maximum(top_s[h], fold(jnp.maximum, s))
        return carry

    lax.fori_loop(lo, hi, scores, 0)
    shift = [jnp.max(top_s[h], axis=1, keepdims=True) * EXP_SCALE for h in range(2)]

    def values(kb, carry):
        v = v_ref[pl.ds(pl.multiple_of(kb * bk, bk), bk), :]
        for h in range(2):
            e = jnp.exp2(s_buf[h, kb] * EXP_SCALE - shift[h])
            sum_s[h] = sum_s[h] + fold(jnp.add, e)
            acc_s[h] = acc_s[h] + mm(e.astype(jnp.bfloat16), v, NN)
        return carry

    lax.fori_loop(lo, hi, values, 0)
    total = [jnp.sum(sum_s[h], axis=1, keepdims=True) for h in range(2)]
    o_ref[:, :] = pair_select(*[acc_s[h] / total[h] for h in range(2)]).astype(jnp.bfloat16)
    lse_ref[:, :] = pair_select(*[shift[h] + jnp.log2(total[h]) for h in range(2)])


def attn_fwd(scal, qkv, doc, n_blocks, bq, bk):
    rows, n_pairs = qkv.shape[0], qkv.shape[1] // 3 // PAIR
    doc_col, doc_row = doc[:, None], doc.reshape(rows // bk, 1, bk)
    n_out = n_blocks * bq
    qspec = pl.BlockSpec((bq, PAIR), lambda i, p, sc: (sc[0] + i, p))
    full = lambda part: pl.BlockSpec((rows, PAIR), lambda i, p, sc: (0, part * n_pairs + p))
    out = pl.BlockSpec((bq, PAIR), lambda i, p, sc: (i, p))
    return pl.pallas_call(
        fwd_body,
        grid_spec=pltpu.PrefetchScalarGridSpec(
            num_scalar_prefetch=1, grid=(n_blocks, n_pairs),
            in_specs=[qspec, full(1), full(2),
                      pl.BlockSpec((bq, 1), lambda i, p, sc: (sc[0] + i, 0)),
                      pl.BlockSpec((rows // bk, 1, bk), lambda i, p, sc: (0, 0, 0))],
            out_specs=[out, out],
            scratch_shapes=[pltpu.VMEM((2, rows // bk, bq, bk), jnp.float32)] + [pltpu.VMEM((2, bq, PAIR), jnp.float32)] * 3),
        out_shape=[jax.ShapeDtypeStruct((n_out, n_pairs * PAIR), jnp.bfloat16),
                   jax.ShapeDtypeStruct((n_out, n_pairs * PAIR), jnp.float32)],
        cost_estimate=cost(4e9),
        name="attn_fwd_global",
    )(scal, qkv, qkv, qkv, doc_col, doc_row)


def stats_body(o_ref, do_ref, lse_ref, out_ref):
    n = o_ref.shape[0]
    lane = lax.broadcasted_iota(jnp.int32, (n, PAIR), 1)
    tile = jnp.zeros((n, PAIR), jnp.float32)
    for p in range(o_ref.shape[1] // PAIR):
        cols = slice(p * PAIR, (p + 1) * PAIR)
        prod = o_ref[:, cols].astype(jnp.float32) * do_ref[:, cols].astype(jnp.float32)
        lse = lse_ref[:, cols]
        for h in range(2):
            delta = jnp.sum(jnp.where(head_lanes((n, PAIR), h), prod, 0.0), axis=1, keepdims=True)
            tile = jnp.where(lane == 8 * p + h, delta, tile)
            tile = jnp.where(lane == 8 * p + 2 + h, lse[:, h * HEAD_DIM:h * HEAD_DIM + 1], tile)
    out_ref[:, :] = tile.T[:out_ref.shape[0], :]


def attn_stats(o, do, lse):
    n, d_model = o.shape
    n_pairs = d_model // PAIR
    return pl.pallas_call(
        stats_body,
        out_shape=jax.ShapeDtypeStruct((8 * n_pairs, n), jnp.float32),
        cost_estimate=cost(1e8),
        name="attn_stats",
    )(o, do, lse)


def local_window(sc_ref, blk, n_blocks):
    i = pl.program_id(0) + sc_ref[0]
    return i * blk, pl.multiple_of(jnp.clip(i - 1, 0, n_blocks - 3) * blk, blk)


def local_fwd_body(blk, n_blocks, sc_ref, q_ref, kv_ref, dq_ref, dk_ref, o_ref, lse_ref):
    d_model = q_ref.shape[1]
    row0, start = local_window(sc_ref, blk, n_blocks)
    ok = window_mask(dq_ref[...], dk_ref[jnp.clip(pl.program_id(0) + sc_ref[0] - 1, 0, n_blocks - 3)], row0, start)
    for p in range(d_model // PAIR):
        cols = slice(p * PAIR, (p + 1) * PAIR)
        q = q_ref[:, cols]
        k = kv_ref[pl.ds(start, 3 * blk), d_model + p * PAIR:d_model + (p + 1) * PAIR]
        v = kv_ref[pl.ds(start, 3 * blk), 2 * d_model + p * PAIR:2 * d_model + (p + 1) * PAIR]
        outs, lses = [], []
        for h in range(2):
            s = jnp.where(ok, mm(keep_head(q, h), k, NT), NEG_BIG)
            top = jnp.max(s, axis=1, keepdims=True)
            e = jnp.exp2((s - top) * EXP_SCALE)
            total = jnp.sum(e, axis=1, keepdims=True)
            outs.append(mm(e.astype(jnp.bfloat16), v, NN) / total)
            lses.append(top * EXP_SCALE + jnp.log2(total))
        o_ref[:, cols] = pair_select(*outs).astype(jnp.bfloat16)
        lse_ref[:, cols] = pair_select(*lses)


def local_docs(doc, blk):
    windows = doc.shape[0] // blk - 2
    return jnp.stack([doc[i * blk:(i + 3) * blk] for i in range(windows)])[:, None, :]


def local_fwd(scal, qkv, doc, n_blocks, blk):
    rows, width = qkv.shape
    d_model = width // 3
    total = rows // blk
    out = pl.BlockSpec((blk, d_model), lambda i, sc: (i, 0))
    return pl.pallas_call(
        functools.partial(local_fwd_body, blk, total),
        grid_spec=pltpu.PrefetchScalarGridSpec(
            num_scalar_prefetch=1, grid=(n_blocks,),
            in_specs=[pl.BlockSpec((blk, d_model), lambda i, sc: (sc[0] + i, 0)),
                      pl.BlockSpec((rows, width), lambda i, sc: (0, 0)),
                      pl.BlockSpec((blk, 1), lambda i, sc: (sc[0] + i, 0)),
                      pl.BlockSpec((total - 2, 1, 3 * blk), lambda i, sc: (0, 0, 0))],
            out_specs=[out, out]),
        out_shape=[jax.ShapeDtypeStruct((n_blocks * blk, d_model), jnp.bfloat16),
                   jax.ShapeDtypeStruct((n_blocks * blk, d_model), jnp.float32)],
        cost_estimate=cost(1e9),
        name="local_fwd",
    )(scal, qkv, qkv, doc[:, None], local_docs(doc, blk))


def local_bwd_body(blk, n_blocks, sc_ref, own_ref, all_ref, o_ref, do_ref, lse_ref, doall_ref, st_ref, dq_ref, dk_ref, cos_ref, sin_ref, out_ref):
    d_model = o_ref.shape[1]
    row0, start = local_window(sc_ref, blk, n_blocks)
    ok = window_mask(dq_ref[...], dk_ref[jnp.clip(pl.program_id(0) + sc_ref[0] - 1, 0, n_blocks - 3)], row0, start)
    cos, sin = cos_ref[...], sin_ref[...]
    near = pl.ds(start, 3 * blk)
    for p in range(d_model // PAIR):
        cols = slice(p * PAIR, (p + 1) * PAIR)
        kcols = slice(d_model + p * PAIR, d_model + (p + 1) * PAIR)
        vcols = slice(2 * d_model + p * PAIR, 2 * d_model + (p + 1) * PAIR)
        q, k, v, do = own_ref[:, cols], own_ref[:, kcols], own_ref[:, vcols], do_ref[:, cols]
        qw, kw, vw, dow = all_ref[near, cols], all_ref[near, kcols], all_ref[near, vcols], doall_ref[near, cols]
        st = st_ref[jnp.clip(pl.program_id(0) + sc_ref[0] - 1, 0, n_blocks - 3), 8 * p:8 * p + 8, :]
        prod = o_ref[:, cols].astype(jnp.float32) * do.astype(jnp.float32)
        dqs, dks, dvs = [], [], []
        for h in range(2):
            delta = jnp.sum(keep_head(prod, h), axis=1, keepdims=True)
            lse = lse_ref[:, p * PAIR + h * HEAD_DIM:p * PAIR + h * HEAD_DIM + 1]
            s = mm(keep_head(q, h), kw, NT)
            prob = jnp.exp2(jnp.where(ok, s * EXP_SCALE - lse, NEG_BIG))
            dp = mm(keep_head(do, h), vw, NT).astype(jnp.bfloat16).astype(jnp.float32)
            dqs.append(mm((prob * (dp - delta)).astype(jnp.bfloat16), kw, NN))
            s = mm(keep_head(k, h), qw, NT)
            prob = jnp.exp2(jnp.where(ok, s * EXP_SCALE - st[2 + h:3 + h, :], NEG_BIG))
            dvs.append(mm(prob.astype(jnp.bfloat16), dow, NN))
            dp = mm(keep_head(v, h), dow, NT).astype(jnp.bfloat16).astype(jnp.float32)
            dks.append(mm((prob * (dp - st[h:h + 1, :])).astype(jnp.bfloat16), qw, NN))
        out_ref[:, cols] = rope_back((pair_select(*dqs) * SCALE).astype(jnp.bfloat16), cos, sin)
        out_ref[:, kcols] = rope_back((pair_select(*dks) * SCALE).astype(jnp.bfloat16), cos, sin)
        out_ref[:, vcols] = pair_select(*dvs).astype(jnp.bfloat16)


def local_bwd(scal, qkv, o, do, lse, stats, doc, cos, sin, n_blocks, blk):
    rows, width = qkv.shape
    d_model = width // 3
    total = rows // blk
    own = pl.BlockSpec((blk, d_model), lambda i, sc: (sc[0] + i, 0))
    table = pl.BlockSpec((blk, PAIR), lambda i, sc: (sc[0] + i, 0))
    whole = lambda w: pl.BlockSpec((rows, w), lambda i, sc: (0, 0))
    st = jnp.stack([stats[:, i * blk:(i + 3) * blk] for i in range(total - 2)])
    return pl.pallas_call(
        functools.partial(local_bwd_body, blk, total),
        grid_spec=pltpu.PrefetchScalarGridSpec(
            num_scalar_prefetch=1, grid=(n_blocks,),
            in_specs=[pl.BlockSpec((blk, width), lambda i, sc: (sc[0] + i, 0)), whole(width), own, own, own, whole(d_model),
                      pl.BlockSpec(st.shape, lambda i, sc: (0, 0, 0)),
                      pl.BlockSpec((blk, 1), lambda i, sc: (sc[0] + i, 0)),
                      pl.BlockSpec((total - 2, 1, 3 * blk), lambda i, sc: (0, 0, 0)), table, table],
            out_specs=pl.BlockSpec((blk, width), lambda i, sc: (i, 0))),
        out_shape=jax.ShapeDtypeStruct((n_blocks * blk, width), jnp.bfloat16),
        cost_estimate=cost(2e9),
        name="local_bwd",
    )(scal, qkv, qkv, o, do, lse, do, st, doc[:, None], local_docs(doc, blk), cos, sin)


STEP_AXIS = {'c': ('dp', 1), 'x': ('dp', 2), 'y': ('dp', 4), 'Z': ('sp', 2), 'z': ('sp', 1)}
A_WAY, B_WAY, C_WAY = 'cxyzZ', 'cyxzZ', 'czZxy'


def partner_of(step):
    axis, bit = STEP_AXIS[step]
    me = lax.axis_index(axis)
    low = (me // bit) % 2
    return {axis: me + bit - 2 * bit * low}, low


def plan_chunks(shapes, ways, splits):
    by_way = {way: [] for way in (A_WAY, B_WAY, C_WAY)}
    for idx, ((rows, cols), part_ways, n_split) in enumerate(zip(shapes, ways, splits)):
        parts = len(part_ways)
        for part, way in enumerate(part_ways):
            for c in range(n_split):
                by_way[way].append((idx, part * rows // parts, rows // parts, cols // n_split, way, pl.ds(c * (cols // n_split), cols // n_split)))
    return [chunk for group in zip(*by_way.values()) for chunk in group]


BWD_WAYS = ((A_WAY, A_WAY), (B_WAY, B_WAY), (C_WAY,), (C_WAY,), (A_WAY, B_WAY), (C_WAY,))
TAIL_WAYS = ((A_WAY, B_WAY), (C_WAY, C_WAY))
STAGGER = 1
MESH_ID = pl.DeviceIdType.MESH
N_STEPS = len(A_WAY)


def greet(peers):
    barrier = pltpu.get_barrier_semaphore()
    for peer in peers:
        pl.semaphore_signal(barrier, inc=1, device_id=peer, device_id_type=MESH_ID)
    pl.semaphore_wait(barrier, len(peers))


def sum_waves(chunks, ins, outs, scratch):
    n_ch = len(chunks)
    lands, works, (load_sem, send_sem, recv_sem) = scratch[:n_ch], scratch[n_ch:2 * n_ch], scratch[2 * n_ch:]
    loads = [pltpu.make_async_copy(ins[idx].at[pl.ds(first, rows), cols], works[j], load_sem.at[j])
             for j, (idx, first, rows, _, _, cols) in enumerate(chunks)]
    for copy in loads:
        copy.start()
    base = [0] * n_ch
    size = [c[2] for c in chunks]
    land_at = [0] * n_ch
    pending = [None] * n_ch

    def advance(j, s):
        idx, first, _, _, way, cols = chunks[j]
        out = outs[idx]
        if s == 0:
            loads[j].wait()
        else:
            copy, keep, half, at = pending[j]
            copy.wait()
            if s <= N_STEPS:
                @pl.loop(0, half // 8)
                def _(r):
                    rows = pl.ds(pl.multiple_of(keep + r * 8, 8), 8)
                    total = works[j][rows, :] + lands[j][pl.ds(pl.multiple_of(at + r * 8, 8), 8), :]
                    if s < N_STEPS:
                        works[j][rows, :] = total
                    else:
                        out[pl.ds(pl.multiple_of(first + keep + r * 8, 8), 8), cols] = total
        if s == 2 * N_STEPS:
            return
        peer, low = partner_of((way + way[::-1])[s])
        if s < N_STEPS:
            half = size[j] // 2
            give = pl.multiple_of(base[j] + (1 - low) * half, 8)
            keep = pl.multiple_of(base[j] + low * half, 8)
            source, target = works[j].at[pl.ds(give, half)], lands[j].at[pl.ds(land_at[j], half)]
            after = (keep, half, land_at[j])
            land_at[j] += half
            base[j], size[j] = keep, half
        else:
            rows = pl.ds(pl.multiple_of(first + base[j], 8), size[j])
            source = target = out.at[rows, cols]
            after = (None, None, None)
            base[j] = pl.multiple_of(base[j] - low * size[j], 8)
            size[j] *= 2
        copy = pltpu.make_async_remote_copy(
            src_ref=source, dst_ref=target, send_sem=send_sem.at[j], recv_sem=recv_sem.at[j, s],
            device_id=peer, device_id_type=MESH_ID)
        copy.start()
        pending[j] = (copy,) + after

    def event(group, s):
        for j in range(3 * group, 3 * group + 3):
            advance(j, s)

    order = sorted((s + group * STAGGER, group, s) for group in range(n_ch // 3) for s in range(2 * N_STEPS + 1))
    return [functools.partial(event, group, s) for _, group, s in order]


def sum_scratch(chunks):
    n_ch = len(chunks)
    dma = pltpu.SemaphoreType.DMA
    return [pltpu.VMEM((c[2], c[3]), jnp.float32) for c in chunks] * 2 + [dma((n_ch,))] * 2 + [dma((n_ch, 2 * N_STEPS))]


def sum_body(chunks, n_arr, *refs):
    ins, gain_in = refs[:n_arr], refs[n_arr]
    outs, (gain_out, gain_land, gsend_sem, grecv_sem) = refs[n_arr + 1:2 * n_arr + 1], refs[2 * n_arr + 1:2 * n_arr + 5]
    waves = sum_waves(chunks, ins, outs, refs[2 * n_arr + 5:])
    greet([partner_of(step)[0] for step in A_WAY])
    gain_out[:, :] = gain_in[:, :]
    pending = []
    for w, wave in enumerate(waves):
        wave()
        if pending:
            pending.pop().wait()
            gain_out[:, :] = gain_out[:, :] + gain_land[w - 1]
        if w < N_STEPS:
            copy = pltpu.make_async_remote_copy(
                src_ref=gain_out, dst_ref=gain_land.at[w], send_sem=gsend_sem.at[w], recv_sem=grecv_sem.at[w],
                device_id=partner_of(A_WAY[w])[0], device_id_type=MESH_ID)
            copy.start()
            pending.append(copy)


def sum_all(grads, gains, collective_id):
    chunks = plan_chunks([g.shape for g in grads], TAIL_WAYS, (2, 1))
    n_arr = len(grads)
    vmem = pl.BlockSpec(memory_space=pltpu.VMEM)
    res = pl.pallas_call(
        functools.partial(sum_body, chunks, n_arr),
        in_specs=[pl.BlockSpec(memory_space=pl.ANY)] * n_arr + [vmem],
        out_specs=[vmem] * (n_arr + 1),
        out_shape=[jax.ShapeDtypeStruct(g.shape, jnp.float32) for g in grads + [gains]],
        scratch_shapes=[pltpu.VMEM((N_STEPS,) + gains.shape, jnp.float32), pltpu.SemaphoreType.DMA((N_STEPS,)),
                        pltpu.SemaphoreType.DMA((N_STEPS,))] + sum_scratch(chunks),
        compiler_params=pltpu.CompilerParams(collective_id=collective_id, has_side_effects=True, vmem_limit_bytes=60 << 20),
        cost_estimate=cost(1e10),
        name="grad_sum",
    )(*grads, gains)
    return res[:-1], res[-1]


def line_rounds(n_dev, ins, outs, send_sem, recv_sem):
    me = lax.axis_index('sp')
    has = (me < n_dev - 1, me > 0)
    arrays = range(len(ins))

    def owner_of(side, d):
        return me - d if side == 0 else me + d

    def exists(side, d):
        return owner_of(0, d) >= 0 if side == 0 else owner_of(1, d) < n_dev

    def copy(side, d, a, source):
        owner = owner_of(side, d)
        return pltpu.make_async_remote_copy(
            src_ref=source if source is not None else outs[a].at[owner], dst_ref=outs[a].at[owner],
            send_sem=send_sem.at[side, d, a], recv_sem=recv_sem.at[side, d, a],
            device_id={'sp': owner_of(side, -1)} if side == 0 else {'sp': me - 1}, device_id_type=MESH_ID)

    def came(side, d, a):
        owner = owner_of(side, d)
        return pltpu.make_async_remote_copy(
            src_ref=outs[a].at[owner], dst_ref=outs[a].at[owner], send_sem=send_sem.at[side, d - 1, a],
            recv_sem=recv_sem.at[side, d - 1, a], device_id={'sp': me}, device_id_type=MESH_ID)

    def first():
        for a in arrays:
            for side in range(2):
                @pl.when(has[side])
                def _():
                    copy(side, 0, a, ins[a]).start()
        for a in arrays:
            outs[a][me] = ins[a][:, :]

    def relay(d):
        for a in arrays:
            for side in range(2):
                @pl.when(exists(side, d))
                def _():
                    came(side, d, a).wait_recv()
                if d < n_dev - 1:
                    @pl.when(exists(side, d) & has[side])
                    def _():
                        copy(side, d, a, None).start()

    def finish():
        for d in range(n_dev - 1):
            for a in arrays:
                for side in range(2):
                    @pl.when(exists(side, d) & has[side])
                    def _():
                        copy(side, d, a, None if d else ins[a]).wait_send()

    return [first] + [functools.partial(relay, d) for d in range(1, n_dev)], finish


def other_shards(n_dev):
    me = lax.axis_index('sp')
    return [{'sp': lax.rem(me + d, n_dev)} for d in range(1, n_dev)]


def gather_qkv_body(n_dev, blk, x_ref, gain_ref, w_ref, cos_ref, sin_ref, out_ref, x_all, send_sem, recv_sem):
    rounds, finish = line_rounds(n_dev, (x_ref,), (x_all,), send_sem, recv_sem)
    me = lax.axis_index('sp')
    n_loc = x_ref.shape[0]
    greet(other_shards(n_dev))

    def shard_qkv(owner):
        @pl.loop(0, n_loc // blk)
        def _(i):
            rows = pl.ds(pl.multiple_of(i * blk, blk), blk)
            table = pl.ds(pl.multiple_of(owner * n_loc + i * blk, blk), blk)

            def put(col, tile):
                out_ref[owner, rows, col:col + tile.shape[1]] = tile

            qkv_tile(x_all[owner, rows, :], gain_ref[:, :], w_ref, cos_ref[table, :], sin_ref[table, :], put)

    rounds[0]()
    shard_qkv(me)
    for d in range(1, n_dev):
        rounds[d]()

        @pl.loop(0, 2)
        def _(side):
            owner = me - d + side * 2 * d

            @pl.when((owner >= 0) & (owner < n_dev))
            def _():
                shard_qkv(owner)
    finish()


def gather_qkv(x, gain, w, cos, sin, n_dev, collective_id):
    vmem = pl.BlockSpec(memory_space=pltpu.VMEM)
    rows, d_model = x.shape
    out = pl.pallas_call(
        functools.partial(gather_qkv_body, n_dev, 256),
        in_specs=[vmem] * 5, out_specs=vmem,
        out_shape=jax.ShapeDtypeStruct((n_dev, rows, 3 * d_model), jnp.bfloat16),
        scratch_shapes=[pltpu.VMEM((n_dev,) + x.shape, x.dtype)] + [pltpu.SemaphoreType.DMA((2, n_dev - 1, 1))] * 2,
        compiler_params=pltpu.CompilerParams(collective_id=collective_id, has_side_effects=True),
        cost_estimate=cost(1e10),
        name="gather_qkv",
    )(x, gain[None, :], w, cos, sin)
    return out.reshape(n_dev * rows, 3 * d_model)


def bwd_body(n_dev, blk, chunks, n_arr, *refs):
    qkv_ref, o_ref, do_ref, lse_ref, st_ref, doc_own, doc_row, cos_ref, sin_ref = refs[:9]
    rest = refs[9:]
    ins, out_ref, outs = rest[:n_arr], rest[n_arr], rest[n_arr + 1:2 * n_arr + 1]
    do_all, st_all, first_s, second_s, lsend, lrecv = rest[2 * n_arr + 1:2 * n_arr + 7]
    waves = sum_waves(chunks, ins, outs, rest[2 * n_arr + 7:])
    rounds, line_done = line_rounds(n_dev, (do_ref, st_ref), (do_all, st_all), lsend, lrecv)
    me = lax.axis_index('sp')
    n_loc, d_model = o_ref.shape
    n_blk = n_dev * n_loc // blk
    per_shard = n_loc // blk
    greet([partner_of(step)[0] for step in 'cxy'] + other_shards(n_dev))
    rounds[0]()

    def tiles(p, i):
        rows = pl.ds(i * blk, blk)
        group = pl.ds(pl.multiple_of(me * n_loc + i * blk, blk), blk)
        cols = [slice(part * d_model + p * PAIR, part * d_model + (p + 1) * PAIR) for part in range(3)]
        return rows, group, cols

    def dq_unit(p, i):
        rows, group, (qc, kc, vc) = tiles(p, i)
        q, do = qkv_ref[group, qc], do_ref[rows, qc]
        prod = o_ref[rows, qc].astype(jnp.float32) * do.astype(jnp.float32)
        qh = [keep_head(q, h) for h in range(2)]
        doh = [keep_head(do, h) for h in range(2)]
        delta = [jnp.sum(keep_head(prod, h), axis=1, keepdims=True) for h in range(2)]
        lse = [lse_ref[rows, p * PAIR + h * HEAD_DIM:p * PAIR + h * HEAD_DIM + 1] for h in range(2)]
        doc = doc_own[rows, :]
        first_s[:, :] = jnp.zeros_like(first_s)

        def step(kb, carry):
            near = pl.ds(pl.multiple_of(kb * blk, blk), blk)
            k, v = qkv_ref[near, kc], qkv_ref[near, vc]
            ok = doc == doc_row[kb]
            parts = []
            for h in range(2):
                prob = jnp.exp2(jnp.where(ok, mm(qh[h], k, NT) * EXP_SCALE - lse[h], NEG_BIG))
                dp = mm(doh[h], v, NT).astype(jnp.bfloat16).astype(jnp.float32)
                parts.append(mm((prob * (dp - delta[h])).astype(jnp.bfloat16), k, NN))
            first_s[:, :] += pair_select(*parts)
            return carry

        lax.fori_loop(0, n_blk // 2, step, 0)
        yield
        lax.fori_loop(n_blk // 2, n_blk, step, 0)
        out_ref[rows, qc] = rope_back((first_s[:, :] * SCALE).astype(jnp.bfloat16), cos_ref[rows, :], sin_ref[rows, :])
        yield

    def dkv_unit(p, i):
        rows, group, (qc, kc, vc) = tiles(p, i)
        kh = [keep_head(qkv_ref[group, kc], h) for h in range(2)]
        vh = [keep_head(qkv_ref[group, vc], h) for h in range(2)]
        doc = doc_own[rows, :]
        first_s[:, :] = jnp.zeros_like(first_s)
        second_s[:, :] = jnp.zeros_like(second_s)

        def step(qb, carry):
            near = pl.ds(pl.multiple_of(qb * blk, blk), blk)
            part = pl.ds(pl.multiple_of(qb % per_shard * blk, blk), blk)
            q, do = qkv_ref[near, qc], do_all[qb // per_shard, part, qc]
            st = st_all[qb // per_shard, 8 * p:8 * p + 8, part]
            ok = doc == doc_row[qb]
            dks, dvs = [], []
            for h in range(2):
                prob = jnp.exp2(jnp.where(ok, mm(kh[h], q, NT) * EXP_SCALE - st[2 + h:3 + h, :], NEG_BIG))
                dvs.append(mm(prob.astype(jnp.bfloat16), do, NN))
                dp = mm(vh[h], do, NT).astype(jnp.bfloat16).astype(jnp.float32)
                dks.append(mm((prob * (dp - st[h:h + 1, :])).astype(jnp.bfloat16), q, NN))
            first_s[:, :] += pair_select(*dks)
            second_s[:, :] += pair_select(*dvs)
            return carry

        lax.fori_loop(0, n_blk // 2, step, 0)
        yield
        lax.fori_loop(n_blk // 2, n_blk, step, 0)
        out_ref[rows, kc] = rope_back((first_s[:, :] * SCALE).astype(jnp.bfloat16), cos_ref[rows, :], sin_ref[rows, :])
        out_ref[rows, vc] = second_s[:, :].astype(jnp.bfloat16)
        yield

    where = [(p, i) for p in range(d_model // PAIR) for i in range(per_shard)]
    units = [functools.partial(dq_unit, *at) for at in where] + [functools.partial(dkv_unit, *at) for at in where]
    slots, turn = 2 * len(units), 0
    for n, unit in enumerate(units):
        if n == len(where):
            rounds[-1]()
        for half, _ in enumerate(unit()):
            if half and n % 2 and n // 2 + 1 < len(rounds) - 1:
                rounds[n // 2 + 1]()
            while turn < len(waves) and turn * slots <= (2 * n + half) * len(waves):
                waves[turn]()
                turn += 1
    for wave in waves[turn:]:
        wave()
    line_done()


def bwd_global(qkv, o, do, lse, stats, doc_own, doc_row, cos, sin, grads, n_dev, blk, collective_id):
    n_grads = len(grads)
    chunks = plan_chunks([g.shape for g in grads], BWD_WAYS, (1,) * n_grads)
    n_arr = len(grads)
    vmem = pl.BlockSpec(memory_space=pltpu.VMEM)
    n_loc, d_model = o.shape
    dma = pltpu.SemaphoreType.DMA
    res = pl.pallas_call(
        functools.partial(bwd_body, n_dev, blk, chunks, n_arr),
        in_specs=[vmem] * 9 + [pl.BlockSpec(memory_space=pl.ANY)] * n_arr,
        out_specs=[vmem] * (n_arr + 1),
        out_shape=[jax.ShapeDtypeStruct((n_loc, 3 * d_model), jnp.bfloat16)]
        + [jax.ShapeDtypeStruct(g.shape, jnp.float32) for g in grads],
        scratch_shapes=[pltpu.VMEM((n_dev,) + do.shape, do.dtype), pltpu.VMEM((n_dev,) + stats.shape, jnp.float32)]
        + [pltpu.VMEM((blk, PAIR), jnp.float32)] * 2 + [dma((2, n_dev - 1, 2))] * 2 + sum_scratch(chunks),
        compiler_params=pltpu.CompilerParams(collective_id=collective_id, has_side_effects=True, vmem_limit_bytes=63 << 20),
        cost_estimate=cost(1e10),
        name="bwd_global",
    )(qkv, o, do, lse, stats, doc_own, doc_row, cos, sin, *grads)
    return res[0], res[1:]


def weight_grad(left_rows, right_rows):
    return lax.dot_general(left_rows, right_rows, (((0,), (0,)), ((), ())), preferred_element_type=jnp.float32)


def input_grad(grad_rows, weight):
    return lax.dot_general(grad_rows, weight, (((1,), (1,)), ((), ())), preferred_element_type=jnp.float32).astype(jnp.bfloat16)


def solution(mesh):
    sp_size, dp_size = mesh.shape['sp'], mesh.shape['dp']
    token_spec = P(('dp', 'sp'), None)
    up_perm = [(i, i + 1) for i in range(sp_size - 1)]
    down_perm = [(i + 1, i) for i in range(sp_size - 1)]

    def with_halo(rows):
        left = lax.ppermute(rows[-HALO:], 'sp', up_perm)
        right = lax.ppermute(rows[:HALO], 'sp', down_perm)
        return jnp.concatenate([left, rows, right], axis=0)

    def device_step(x_loc, cu_loc, pos_loc, w_qkv, w_proj, w_up, w_down, ln_attn, ln_mlp, d_out):
        n_loc, d_model = x_loc.shape
        n_group = n_loc * sp_size
        me = lax.axis_index('sp')
        cu = cu_loc[0]
        tok = jnp.arange(n_group)
        doc_all = jnp.sum((cu[None, 1:-1] <= tok[:, None]).astype(jnp.int32), axis=1)
        start_of = lambda at: jnp.max(jnp.where(cu[None, :-1] <= at[:, None], cu[None, :-1], 0), axis=1)
        end_of = lambda at: jnp.min(jnp.where(cu[None, 1:] > at[:, None], cu[None, 1:], n_group), axis=1)
        pos_all = tok - start_of(tok)
        tok_ext = me * n_loc - HALO + jnp.arange(n_loc + 2 * HALO)
        inside = (tok_ext >= 0) & (tok_ext < n_group)
        doc_at = jnp.sum((cu[None, 1:-1] <= tok_ext[:, None]).astype(jnp.int32), axis=1)
        doc_ext = jnp.where(inside, doc_at, -1)
        pos_ext = jnp.where(inside, tok_ext - start_of(tok_ext), 0)

        def bounds(blk, other):
            first = me * n_loc + jnp.arange(n_loc // blk) * blk
            lo = start_of(first) // other
            hi = (end_of(first + blk - 1) + other - 1) // other
            pairs = jnp.stack([lo, hi], axis=1).reshape(-1)
            return jnp.concatenate([(me * n_loc // blk)[None], pairs]).astype(jnp.int32)

        sc_q = bounds(BQ_GLOBAL, BK_GLOBAL)
        n_ext = n_loc // BLK_LOCAL + 2 * (HALO // BLK_LOCAL)

        cos0, sin0 = rope_tables(pos_all, BASES[0])
        cos1, sin1 = rope_tables(pos_ext, BASES[1])

        def mlp_forward(x_rows, att, layer):
            x_mid = (x_rows.astype(jnp.float32) + jnp.dot(att, w_proj[layer], preferred_element_type=jnp.float32)).astype(jnp.bfloat16)
            h_mlp, ln2_pull = jax.vjp(layer_norm, x_mid, ln_mlp[layer])
            up_rows = jnp.dot(h_mlp, w_up[layer], preferred_element_type=jnp.float32).astype(jnp.bfloat16)
            act_rows, act_pull = jax.vjp(geglu, up_rows)
            y_rows = (x_mid.astype(jnp.float32) + jnp.dot(act_rows, w_down[layer], preferred_element_type=jnp.float32)).astype(jnp.bfloat16)
            return y_rows, (h_mlp, ln2_pull, act_pull, act_rows)

        def mlp_backward(d_y, saved, att, layer):
            h_mlp, ln2_pull, act_pull, act_rows = saved
            (d_up,) = act_pull(input_grad(d_y, w_down[layer]))
            d_mid_ln, g_ln = ln2_pull(input_grad(d_up, w_up[layer]))
            d_mid = d_y + d_mid_ln
            d_att = input_grad(d_mid, w_proj[layer])
            grads = (weight_grad(act_rows, d_y), weight_grad(h_mlp, d_up), weight_grad(att, d_mid))
            return d_mid, d_att, grads, g_ln

        qkv0 = gather_qkv(x_loc, ln_attn[0], w_qkv[0], cos0, sin0, sp_size, 0)
        att0, lse0 = attn_fwd(sc_q, qkv0, doc_all, n_loc // BQ_GLOBAL, BQ_GLOBAL, BK_GLOBAL)
        y0, saved0 = mlp_forward(x_loc, att0, 0)
        qkv1 = qkv_rope(with_halo(y0), ln_attn[1], w_qkv[1], cos1, sin1)
        att1x, lse1 = local_fwd(jnp.zeros((1,), jnp.int32), qkv1, doc_ext, n_ext, BLK_LOCAL)
        att1 = att1x[HALO:HALO + n_loc]
        y1, saved1 = mlp_forward(y0, att1, 1)

        def finish(d_qkv, x_rows, d_mid, layer):
            h_attn, ln1_pull = jax.vjp(layer_norm, x_rows, ln_attn[layer])
            g_qkv = weight_grad(h_attn, d_qkv)
            d_x_ln, g_ln = ln1_pull(input_grad(d_qkv, w_qkv[layer]))
            return d_mid + d_x_ln, g_qkv, g_ln

        d_mid1, d_att1, (g_down1, g_up1, g_proj1), g_lnm1 = mlp_backward(d_out, saved1, att1, 1)
        do_ext = with_halo(d_att1)
        stats1 = attn_stats(att1x, do_ext, lse1)
        d_qkv1 = local_bwd(jnp.ones((1,), jnp.int32), qkv1, att1x, do_ext, lse1, stats1, doc_ext, cos1, sin1, n_loc // BLK_LOCAL, BLK_LOCAL)
        d_y0, g_qkv1, g_lna1 = finish(d_qkv1, y0, d_mid1, 1)
        d_mid0, d_att0, (g_down0, g_up0, g_proj0), g_lnm0 = mlp_backward(d_y0, saved0, att0, 0)
        stats0 = attn_stats(att0, d_att0, lse0)
        own_rows = lambda table: lax.dynamic_slice_in_dim(table, me * n_loc, n_loc, 0)
        d_qkv0, (qkvg1, up1, down1, proj1, up0, down0) = bwd_global(
            qkv0, att0, d_att0, lse0, stats0, own_rows(doc_all[:, None]), doc_all.reshape(-1, 1, BK_GLOBAL),
            own_rows(cos0), own_rows(sin0), [g_qkv1, g_up1, g_down1, g_proj1, g_up0, g_down0], sp_size, BK_GLOBAL, 1)
        d_x, g_qkv0, g_lna0 = finish(d_qkv0, x_loc, d_mid0, 0)
        gains = jnp.concatenate([jnp.stack([g_lna0, g_lna1, g_lnm0, g_lnm1]), jnp.zeros((4, d_model), jnp.float32)])
        (qkvg0, proj0), gains = sum_all([g_qkv0, g_proj0], gains, 2)
        return (y1, d_x, jnp.stack([qkvg0, qkvg1]), jnp.stack([proj0, proj1]), jnp.stack([up0, up1]),
                jnp.stack([down0, down1]), gains[:2], gains[2:4])

    in_specs = (token_spec, P('dp', None), P(('dp', 'sp')), P(), P(), P(), P(), P(), P(), token_spec)
    out_specs = (token_spec, token_spec, P(), P(), P(), P(), P(), P())
    return jax.shard_map(device_step, mesh=mesh, in_specs=in_specs, out_specs=out_specs, check_vma=False)
```
